32 devices in a mesh: dp: 8 (over y, x, core), mp: 4 (over z).
Axes of the slice: x: 2, y: 2, z: 4, core: 2. Of those that a mesh axis runs over, the one named last changes fastest.
Arguments:
- hidden: bfloat16 [16384, 13824], P('dp', 'mp'), may hold values from -6 to 6
- out_grad: bfloat16 [16384, 5120], P('dp', 'mp'), may hold values from -6 to 6
- proj_in: bfloat16 [64, 13824], P(None, 'mp'), may hold values from -0.0546875 to 0.0546875
- proj_out: bfloat16 [64, 5120], P(None, 'mp'), may hold values from -0.078125 to 0.078125
- segment_ids: int32 [8, 2048], P('dp'), may hold values from 0 to 15, never falling along the last dimension, each value on 1 to 1024 neighbouring positions
Outputs:
- features: float32 [128, 4096], P('dp')
- gram: float32 [4096, 4096], P(('dp', 'mp'))
The draws below stay inside these ranges and needn't reach their ends.
Inputs may be any that keep to these rules, and one draw needn't show every extreme that they name: `segment_ids`: within each row the numbers never fall; each of the 16 numbers names 1 to 1024 tokens of the row.
All inputs are finite; a program needn't handle non-finite values.
Results may differ from the reference program's by a relative error of at most 0.0003.
Values sent between devices are 32-bit elements; how exact they have to be, the bound alone decides.
No kernel may reach another device: no remote copies, remote signals or barrier semaphores. Data moves between devices by JAX's collectives and lax.ppermute only.
A program may use at most 64 MiB of HBM per device.

```python
import math
import jax
import jax.numpy as jnp
import numpy as np
from jax import lax

D = 5120
FF = 13824
RANK = 64
TOK_DEV = 2048
EX_DEV = 16
PROJ = 4096
TOKENS = 16384
EXAMPLES = 128
N_DP = 8


def block_scale(rng, extent, pieces, least, largest):
    def one(dim, parts):
        heights = jax.random.uniform(jax.random.fold_in(jax.random.fold_in(rng, 6), dim), (parts,), jnp.float32, least / len(pieces), largest / len(pieces))
        return jnp.repeat(jnp.exp(heights), extent[dim] // parts).reshape((-1,) + (1,) * (len(extent) - dim - 1))

    level = one(*pieces[0])
    for cut in pieces[1:]:
        level = level * one(*cut)
    return level


def split_up(count, total, bound, lean):
    loads = [(1 << 20) // math.isqrt(rank ** lean) + 1 for rank in range(2, count + 1)]
    spare, given = total - bound - (count - 1), [1] * (count - 1)
    while spare > 0:
        movable = [i for i in range(count - 1) if given[i] < bound]
        pool, remaining = sum([loads[i] for i in movable]), spare
        for i in movable:
            addition = min(bound - given[i], max(1, remaining * loads[i] // pool), spare)
            given[i] = given[i] + addition
            spare = spare - addition
    return np.array([bound] + given)


def ragged(rng, amount, total, limit, slope):
    if amount == 2:
        one = jax.random.randint(rng, (), max(1, total - limit), min(limit, total - 1) + 1)
        return jnp.stack([one, total - one])
    sizes = jnp.asarray(split_up(amount, total, limit, slope), jnp.int32)
    pairs = (amount - 1) // 2
    source_of, receiver = sizes[1:1 + 2 * pairs:2], sizes[2:2 + 2 * pairs:2]
    slack = jnp.minimum(source_of - 1, limit - receiver)
    passed = jax.random.randint(jax.random.fold_in(rng, 1), (pairs,), 0, 1 << 20) % (slack + 1)
    sizes = sizes.at[1:1 + 2 * pairs:2].set(source_of - passed).at[2:2 + 2 * pairs:2].set(receiver + passed)
    return sizes[jax.random.permutation(jax.random.fold_in(rng, 2), amount)]


def noise(rng, shape, width, most, pieces=(), held_as=jnp.bfloat16):
    loudness = block_scale(rng, shape, pieces, -0.22, 0.18) if pieces else 1.0
    entries = jax.random.normal(rng, shape, jnp.float32) * width * loudness
    return jnp.minimum(jnp.maximum(entries, -most), most).astype(held_as)


def setup_inputs(seed: int = 0) -> dict:
    key_list = jax.random.split(jax.random.key(seed), 6)
    hidden = noise(key_list[0], (TOKENS, FF), 1.0, 6.0, ((0, 8), (1, 4)))
    out_grad = noise(key_list[1], (TOKENS, D), 1.0, 6.0, ((0, 8), (1, 4)))
    proj_in = noise(key_list[2], (RANK, FF), FF ** -0.5, 0.0546875, ((1, 4),))
    proj_out = noise(key_list[3], (RANK, D), D ** -0.5, 0.078125, ((1, 4),))
    segment_ids = jax.vmap(lambda own: jnp.searchsorted(jnp.cumsum(ragged(own, EX_DEV, TOK_DEV, TOK_DEV // 2, 2)), jnp.arange(TOK_DEV), side="right"))(jax.random.split(key_list[4], N_DP)).reshape((N_DP, TOK_DEV)).astype(jnp.int32)
    return dict(hidden=hidden, out_grad=out_grad, proj_in=proj_in, proj_out=proj_out, segment_ids=segment_ids)


def example_grads(example_ids, inputs, outputs, examples):
    onehot = (example_ids[None, :] == jnp.arange(examples, dtype=jnp.int32)[:, None]).astype(jnp.float32)
    counts = lax.optimization_barrier(jnp.sum(onehot, axis=1))
    weighted = onehot[:, :, None] * outputs[None, :, :]
    grads = jnp.einsum('eti,tj->eij', weighted, inputs, precision=lax.Precision.HIGHEST)
    return grads.reshape(examples, -1) / jnp.sqrt(counts)[:, None]

def reference(hidden, out_grad, proj_in, proj_out, segment_ids):
    hidden_rows = hidden.reshape(N_DP, TOK_DEV, FF)
    grad_rows = out_grad.reshape(N_DP, TOK_DEV, D)

    def per_sequence(operands):
        hidden_row, grad_row, ids_row = operands
        inputs = lax.dot_general(hidden_row, proj_in, (((1,), (1,)), ((), ())), preferred_element_type=jnp.float32)
        outputs = lax.dot_general(grad_row, proj_out, (((1,), (1,)), ((), ())), preferred_element_type=jnp.float32)
        return example_grads(ids_row, inputs, outputs, EX_DEV)
    features = lax.map(per_sequence, (hidden_rows, grad_rows, segment_ids)).reshape(EXAMPLES, PROJ)
    gram = lax.dot_general(features, features, (((0,), (0,)), ((), ())), precision=lax.Precision.HIGHEST, preferred_element_type=jnp.float32) / EXAMPLES
    return (features, gram)
```

```python
import functools

import jax
import jax.numpy as jnp
from jax import lax
from jax.experimental import pallas as pl
from jax.experimental.pallas import tpu as pltpu
from jax.sharding import PartitionSpec as P


EX_DEV = 16
NT = (((1,), (1,)), ((), ()))
HBM = pl.BlockSpec(memory_space=pltpu.HBM)
VMEM = pl.BlockSpec(memory_space=pltpu.VMEM)
SMEM = pl.BlockSpec(memory_space=pltpu.SMEM)


def in_hbm(x):
    return pltpu.with_memory_space_constraint(x, pltpu.HBM)


def in_vmem(x):
    return pltpu.with_memory_space_constraint(x, pltpu.VMEM)


def project_kernel(rows, x_ref, w_ref, out_ref, x_buf, w_buf, x_sem, w_sem):
    n = x_buf.shape[0]
    weights = pltpu.make_async_copy(w_ref, w_buf, w_sem)
    weights.start()
    halves = 2 if rows % 2 == 0 else 1
    size = rows // halves
    copies = [
        [
            pltpu.make_async_copy(
                x_ref.at[pl.ds(i * rows + h * size, size)],
                x_buf.at[i, pl.ds(h * size, size)],
                x_sem.at[i, h],
            )
            for h in range(halves)
        ]
        for i in range(n)
    ]

    def start(i):
        if i < n:
            for copy in copies[i]:
                copy.start()

    start(0)
    weights.wait()
    copies[0][0].wait()
    start(1)
    for copy in copies[0][1:]:
        copy.wait()
    for i in range(n):
        if i > 0:
            for copy in copies[i]:
                copy.wait()
        start(i + 2 if i > 0 else 2)
        out_ref[:, i * rows : (i + 1) * rows] = lax.dot_general(
            w_buf[...], x_buf[i], NT, preferred_element_type=jnp.float32
        )


def project(x, w, rows):
    tokens, depth = x.shape
    width = w.shape[0]
    rows = rows if tokens % rows == 0 else tokens
    n = tokens // rows
    return pl.pallas_call(
        functools.partial(project_kernel, rows),
        in_specs=[HBM, HBM],
        out_specs=VMEM,
        out_shape=pltpu.VMEM((width, tokens), jnp.float32),
        scratch_shapes=[
            pltpu.VMEM((n, rows, depth), x.dtype),
            pltpu.VMEM((width, depth), w.dtype),
            pltpu.SemaphoreType.DMA((n, 2)),
            pltpu.SemaphoreType.DMA,
        ],
        cost_estimate=pl.CostEstimate(
            flops=2 * tokens * depth * width,
            bytes_accessed=2 * tokens * depth,
            transcendentals=0,
        ),
        compiler_params=pltpu.CompilerParams(vmem_limit_bytes=24 << 20),
        name="project",
    )(in_hbm(x), in_hbm(w))


def split(x):
    high = x.astype(jnp.bfloat16)
    return high, (x - high.astype(jnp.float32)).astype(jnp.bfloat16)


def total(refs):
    return sum((r[...] for r in refs[1:]), refs[0][...])


def expand_kernel(n, examples, seg_ref, *refs):
    out_ref, scale_ref = refs[n:]
    tokens = seg_ref.shape[1]
    outputs = total(refs[:n])
    mask = (
        seg_ref[...] == lax.broadcasted_iota(jnp.int32, (examples, tokens), 0)
    ).astype(jnp.float32)
    high = outputs.astype(jnp.bfloat16).astype(jnp.float32)
    low = outputs - high
    width = outputs.shape[0]
    half = width * examples
    for i in range(width):
        first = i * examples
        rows = slice(first, first + examples)
        out_ref[rows, :] = (high[i : i + 1, :] * mask).astype(jnp.bfloat16)
        rows = slice(half + first, half + first + examples)
        out_ref[rows, :] = (low[i : i + 1, :] * mask).astype(jnp.bfloat16)
    scale_ref[...] = jnp.broadcast_to(
        1.0 / jnp.sqrt(jnp.sum(mask, axis=1, keepdims=True)), scale_ref.shape
    )


def expand(segment_ids, parts, examples):
    width, tokens = parts[0].shape
    n = len(parts)
    return pl.pallas_call(
        functools.partial(expand_kernel, n, examples),
        in_specs=[VMEM] * (1 + n),
        out_specs=[VMEM] * 2,
        out_shape=[
            pltpu.VMEM((2 * width * examples, tokens), jnp.bfloat16),
            pltpu.VMEM((examples, 128), jnp.float32),
        ],
        cost_estimate=pl.CostEstimate(
            flops=4 * width * examples * tokens,
            bytes_accessed=4 * width * examples * tokens,
            transcendentals=0,
        ),
        compiler_params=pltpu.CompilerParams(vmem_limit_bytes=24 << 20),
        name="expand",
    )(segment_ids, *parts)


def outer_kernel(n, examples, left_ref, scale_ref, *refs):
    input_refs, out_refs = refs[:n], refs[n:]
    width = input_refs[0].shape[0]
    right = jnp.concatenate(split(total(input_refs)), axis=0)
    scale = scale_ref[:, :width]
    half = width * examples
    rank = width // len(out_refs)
    rows = rank * examples
    for k, out_ref in enumerate(out_refs):

        def dot(first):
            return lax.dot_general(
                left_ref[first : first + rows, :], right, NT, preferred_element_type=jnp.float32
            )

        high, low = dot(k * rows), dot(half + k * rows)
        sums = high[:, :width] + high[:, width:] + low[:, :width]
        for i in range(rank):
            out_ref[:, i * width : (i + 1) * width] = (
                sums[i * examples : (i + 1) * examples] * scale
            )


def outer_sums(left, scale, inputs, cuts):
    examples = scale.shape[0]
    rows, tokens = left.shape
    width = inputs[0].shape[0]
    n = len(inputs)
    return pl.pallas_call(
        functools.partial(outer_kernel, n, examples),
        in_specs=[VMEM] * (2 + n),
        out_specs=[VMEM] * cuts,
        out_shape=[pltpu.VMEM((examples, width * width // cuts), jnp.float32)] * cuts,
        cost_estimate=pl.CostEstimate(
            flops=4 * rows * tokens * width,
            bytes_accessed=2 * rows * tokens,
            transcendentals=0,
        ),
        compiler_params=pltpu.CompilerParams(vmem_limit_bytes=24 << 20),
        name="outer_sums",
    )(in_vmem(left), in_vmem(scale), *inputs)


def gram_kernel(n, cuts, row_count, examples, block, first_ref, *refs):
    parts = refs[: n * cuts]
    features_ref, out_ref, terms, rows_ref, out_sem = refs[n * cuts :]
    size = parts[0].shape[1]
    total_examples = n * examples
    for k in range(n):
        high = slice(k * examples, (k + 1) * examples)
        low = slice(total_examples + k * examples, total_examples + (k + 1) * examples)
        for c in range(cuts):
            columns = slice(c * size, (c + 1) * size)
            part = parts[k * cuts + c][...]
            if k == 0:
                features_ref[:, columns] = part
            terms[high, columns], terms[low, columns] = split(part)
    lanes = rows_ref.shape[0]
    first = first_ref[0]
    base = pl.multiple_of(first // lanes * lanes, lanes)
    left_high = terms[:total_examples, pl.ds(base, lanes)].T
    left_low = terms[total_examples:, pl.ds(base, lanes)].T
    left_twice = jnp.concatenate([left_high, left_high], axis=1)
    offset = pl.multiple_of(first - base, row_count)

    def dot(a, b):
        return lax.dot_general(
            a, b, (((1,), (0,)), ((), ())), preferred_element_type=jnp.float32
        )

    copies = []
    for k in range(out_ref.shape[1] // block):
        columns = slice(k * block, (k + 1) * block)
        product = dot(left_twice, terms[:, columns]) + dot(
            left_low, terms[:total_examples, columns]
        )
        rows_ref[:, columns] = product * (1.0 / total_examples)
        copies.append(
            pltpu.make_async_copy(
                rows_ref.at[pl.ds(offset, row_count), columns], out_ref.at[:, columns], out_sem.at[k]
            )
        )
        copies[-1].start()
    for copy in copies:
        copy.wait()


def gram_rows(first, parts, row_count):
    n, cuts = len(parts), len(parts[0])
    examples = parts[0][0].shape[0]
    size = sum(x.shape[1] for x in parts[0])
    block = size // 4 if size % 512 == 0 else size
    return pl.pallas_call(
        functools.partial(gram_kernel, n, cuts, row_count, examples, block),
        in_specs=[SMEM] + [VMEM] * (n * cuts),
        out_specs=[VMEM, HBM],
        out_shape=[
            jax.ShapeDtypeStruct((examples, size), jnp.float32),
            jax.ShapeDtypeStruct((row_count, size), jnp.float32),
        ],
        scratch_shapes=[
            pltpu.VMEM((2 * n * examples, size), jnp.bfloat16),
            pltpu.VMEM((max(row_count, 128), size), jnp.float32),
            pltpu.SemaphoreType.DMA((size // block,)),
        ],
        cost_estimate=pl.CostEstimate(
            flops=6 * n * examples * row_count * size,
            bytes_accessed=4 * (n * examples + row_count) * size,
            transcendentals=0,
        ),
        compiler_params=pltpu.CompilerParams(vmem_limit_bytes=40 << 20),
        name="gram_rows",
    )(first, *[x for piece in parts for x in piece])


def body(hidden, out_grad, proj_in, proj_out, segment_ids):
    width = proj_in.shape[0]
    proj_size = width * width
    data = lax.axis_size("dp")
    model = lax.axis_size("mp")
    row_count = proj_size // (data * model)
    axes = ("dp", "mp")
    pair = 2 if data % 2 == 0 else 1
    groups = data // pair

    def owner(d):
        return min((model - 1) // 2 + d % pair, model - 1)

    def at(d, m):
        return d * model + (owner(d) + m) % model

    def hops(m):
        return max(abs((owner(d) + m) % model - owner(d)) for d in range(pair))

    others = sorted(range(1, model), key=hops)

    def to_owner(x):
        return [x] + [
            lax.ppermute(x, axes, [(at(d, m), at(d, 0)) for d in range(data)])
            for m in others
        ]

    def from_owner(x):
        return [
            lax.ppermute(x, axes, [(at(d, 0), at(d, m)) for d in range(data)])
            for m in others
        ]

    def other(g, k):
        return g ^ k if groups & (groups - 1) == 0 else (g + k) % groups

    def across(x, k):
        return lax.ppermute(
            x,
            "dp",
            [
                (g * pair + c, other(g, k) * pair + c)
                for g in range(groups)
                for c in range(pair)
            ],
        )

    def swap(x):
        return lax.ppermute(x, "dp", [(d, d ^ 1) for d in range(data)])

    d, m = lax.axis_index("dp"), lax.axis_index("mp")
    is_owner = m == jnp.minimum((model - 1) // 2 + d % pair, model - 1)

    outputs = project(out_grad, proj_out, 1024)
    outputs_sent = to_owner(outputs)
    inputs = project(hidden, proj_in, 512)
    inputs_sent = to_owner(inputs)
    left, scale = expand(segment_ids, outputs_sent, EX_DEV)
    pieces = []
    for summed in outer_sums(left, scale, inputs_sent, 2):
        features = jnp.where(is_owner, summed, sum(from_owner(summed)))
        parts = [features] + [across(features, k) for k in range(1, groups)]
        if pair == 2:
            parts = parts + [swap(x) for x in parts]
        pieces.append(parts)
    first = ((d * model + m) * row_count).astype(jnp.int32).reshape(1)
    features, gram = gram_rows(first, list(zip(*pieces)), row_count)
    return features, gram


def solution(mesh):
    placed = (P("dp", "mp"), P("dp", "mp"), P(None, "mp"), P(None, "mp"), P("dp", None))
    return jax.shard_map(
        body,
        mesh=mesh,
        in_specs=placed,
        out_specs=(P("dp", None), P(("dp", "mp"), None)),
        check_vma=False,
    )
```

```python
import functools

import jax
import jax.numpy as jnp
from jax import lax
from jax.experimental import pallas as pl
from jax.experimental.pallas import tpu as pltpu
from jax.sharding import PartitionSpec as P


EX_DEV = 16
NT = (((1,), (1,)), ((), ()))
HBM = pl.BlockSpec(memory_space=pltpu.HBM)
VMEM = pl.BlockSpec(memory_space=pltpu.VMEM)
SMEM = pl.BlockSpec(memory_space=pltpu.SMEM)


def in_hbm(x):
    return pltpu.with_memory_space_constraint(x, pltpu.HBM)


def in_vmem(x):
    return pltpu.with_memory_space_constraint(x, pltpu.VMEM)


def project_kernel(blocks, cuts, x_ref, w_ref, *refs):
    out_refs = refs[: len(cuts)]
    x_buf, w_buf, x_sem, w_sem = refs[len(cuts) :]
    n = len(blocks)
    weights = pltpu.make_async_copy(w_ref, w_buf, w_sem)
    weights.start()
    copies = [
        pltpu.make_async_copy(
            x_ref.at[pl.ds(first, rows)], x_buf.at[pl.ds(first, rows)], x_sem.at[i]
        )
        for i, (first, rows) in enumerate(blocks)
    ]

    for copy in copies[:2]:
        copy.start()
    weights.wait()
    for i, (first, rows) in enumerate(blocks):
        copies[i].wait()
        if i + 2 < n:
            copies[i + 2].start()
        product = lax.dot_general(
            w_buf[...], x_buf[pl.ds(first, rows)], NT, preferred_element_type=jnp.float32
        )
        begin = 0
        for cut, out_ref in zip(cuts, out_refs):
            if begin <= first < begin + cut:
                out_ref[:, first - begin : first - begin + rows] = product
            begin += cut


def project(x, w, blocks, cuts):
    tokens, depth = x.shape
    width = w.shape[0]
    firsts = [sum(blocks[:i]) for i in range(len(blocks))]
    return pl.pallas_call(
        functools.partial(project_kernel, list(zip(firsts, blocks)), cuts),
        in_specs=[HBM, HBM],
        out_specs=[VMEM] * len(cuts),
        out_shape=[pltpu.VMEM((width, cut), jnp.float32) for cut in cuts],
        scratch_shapes=[
            pltpu.VMEM((tokens, depth), x.dtype),
            pltpu.VMEM((width, depth), w.dtype),
            pltpu.SemaphoreType.DMA((len(blocks),)),
            pltpu.SemaphoreType.DMA,
        ],
        cost_estimate=pl.CostEstimate(
            flops=2 * tokens * depth * width,
            bytes_accessed=2 * tokens * depth,
            transcendentals=0,
        ),
        compiler_params=pltpu.CompilerParams(vmem_limit_bytes=24 << 20),
        name="project",
    )(in_hbm(x), in_hbm(w))


def split(x):
    high = x.astype(jnp.bfloat16)
    return high, (x - high.astype(jnp.float32)).astype(jnp.bfloat16)


def total(refs):
    return sum((r[...] for r in refs[1:]), refs[0][...])


def expand_kernel(n, examples, seg_ref, *refs):
    out_ref, scale_ref = refs[n:]
    tokens = seg_ref.shape[1]
    outputs = total(refs[:n])
    mask = (
        seg_ref[...] == lax.broadcasted_iota(jnp.int32, (examples, tokens), 0)
    ).astype(jnp.float32)
    high = outputs.astype(jnp.bfloat16).astype(jnp.float32)
    low = outputs - high
    width = outputs.shape[0]
    half = width * examples
    for i in range(width):
        first = i * examples
        rows = slice(first, first + examples)
        out_ref[rows, :] = (high[i : i + 1, :] * mask).astype(jnp.bfloat16)
        rows = slice(half + first, half + first + examples)
        out_ref[rows, :] = (low[i : i + 1, :] * mask).astype(jnp.bfloat16)
    scale_ref[...] = jnp.broadcast_to(
        1.0 / jnp.sqrt(jnp.sum(mask, axis=1, keepdims=True)), scale_ref.shape
    )


def expand(segment_ids, parts, examples):
    width, tokens = parts[0].shape
    n = len(parts)
    return pl.pallas_call(
        functools.partial(expand_kernel, n, examples),
        in_specs=[VMEM] * (1 + n),
        out_specs=[VMEM] * 2,
        out_shape=[
            pltpu.VMEM((2 * width * examples, tokens), jnp.bfloat16),
            pltpu.VMEM((examples, 128), jnp.float32),
        ],
        cost_estimate=pl.CostEstimate(
            flops=4 * width * examples * tokens,
            bytes_accessed=4 * width * examples * tokens,
            transcendentals=0,
        ),
        compiler_params=pltpu.CompilerParams(vmem_limit_bytes=24 << 20),
        name="expand",
    )(segment_ids, *parts)


def outer_kernel(n, examples, first, last, left_ref, scale_ref, *refs):
    if first > 0:
        before_ref, *refs = refs
    input_refs, out_refs = refs[:n], refs[n:]
    width, tokens = input_refs[0].shape
    right = jnp.concatenate(split(total(input_refs)), axis=0)
    scale = scale_ref[:, :width]
    half = width * examples
    rank = width // len(out_refs)
    rows = rank * examples
    for k, out_ref in enumerate(out_refs):

        def dot(row):
            return lax.dot_general(
                left_ref[row : row + rows, first : first + tokens],
                right,
                NT,
                preferred_element_type=jnp.float32,
            )

        high, low = dot(k * rows), dot(half + k * rows)
        sums = high[:, :width] + high[:, width:] + low[:, :width] + low[:, width:]
        if first > 0:
            sums = sums + before_ref[k * rows : (k + 1) * rows, :]
        if not last:
            out_ref[...] = sums
            continue
        for i in range(rank):
            out_ref[:, i * width : (i + 1) * width] = (
                sums[i * examples : (i + 1) * examples] * scale
            )


def outer_sums(left, scale, inputs, first, before, cuts):
    examples = scale.shape[0]
    rows = left.shape[0]
    width, tokens = inputs[0].shape
    n = len(inputs)
    shapes = [(examples, width * width // cuts)] * cuts if cuts else [(width * examples, width)]
    operands = [left, scale] + ([before] if first > 0 else [])
    return pl.pallas_call(
        functools.partial(outer_kernel, n, examples, first, bool(cuts)),
        in_specs=[VMEM] * (len(operands) + n),
        out_specs=[VMEM] * len(shapes),
        out_shape=[pltpu.VMEM(shape, jnp.float32) for shape in shapes],
        cost_estimate=pl.CostEstimate(
            flops=4 * rows * tokens * width,
            bytes_accessed=2 * rows * tokens,
            transcendentals=0,
        ),
        compiler_params=pltpu.CompilerParams(vmem_limit_bytes=24 << 20),
        name="outer_sums",
    )(*[in_vmem(x) for x in operands], *inputs)


def gram_kernel(n, cuts, row_count, examples, block, first_ref, *refs):
    parts = refs[: n * cuts]
    features_ref, out_ref, terms, rows_ref, out_sem, features_sem = refs[n * cuts :]
    size = parts[0].shape[1]
    total_examples = n * examples
    copies = [
        pltpu.make_async_copy(
            parts[c], features_ref.at[:, pl.ds(c * size, size)], features_sem.at[c]
        )
        for c in range(cuts)
    ]
    for copy in copies:
        copy.start()
    for k in range(n):
        high = slice(k * examples, (k + 1) * examples)
        low = slice(total_examples + k * examples, total_examples + (k + 1) * examples)
        for c in range(cuts):
            columns = slice(c * size, (c + 1) * size)
            terms[high, columns], terms[low, columns] = split(parts[k * cuts + c][...])
    lanes = rows_ref.shape[0]
    first = first_ref[0]
    base = pl.multiple_of(first // lanes * lanes, lanes)
    left_high = terms[:total_examples, pl.ds(base, lanes)].T
    left_low = terms[total_examples:, pl.ds(base, lanes)].T
    left_twice = jnp.concatenate([left_high, left_high], axis=1)
    offset = pl.multiple_of(first - base, row_count)

    def dot(a, b):
        return lax.dot_general(
            a, b, (((1,), (0,)), ((), ())), preferred_element_type=jnp.float32
        )

    for k in range(out_ref.shape[1] // block):
        columns = slice(k * block, (k + 1) * block)
        product = dot(left_twice, terms[:, columns]) + dot(
            left_low, terms[:total_examples, columns]
        )
        rows_ref[:, columns] = product * (1.0 / total_examples)
        copies.append(
            pltpu.make_async_copy(
                rows_ref.at[pl.ds(offset, row_count), columns], out_ref.at[:, columns], out_sem.at[k]
            )
        )
        copies[-1].start()
    for copy in copies:
        copy.wait()


def gram_rows(first, parts, row_count):
    n, cuts = len(parts), len(parts[0])
    examples = parts[0][0].shape[0]
    size = sum(x.shape[1] for x in parts[0])
    block = size // 4 if size % 512 == 0 else size
    return pl.pallas_call(
        functools.partial(gram_kernel, n, cuts, row_count, examples, block),
        in_specs=[SMEM] + [VMEM] * (n * cuts),
        out_specs=[HBM, HBM],
        out_shape=[
            jax.ShapeDtypeStruct((examples, size), jnp.float32),
            jax.ShapeDtypeStruct((row_count, size), jnp.float32),
        ],
        scratch_shapes=[
            pltpu.VMEM((2 * n * examples, size), jnp.bfloat16),
            pltpu.VMEM((max(row_count, 128), size), jnp.float32),
            pltpu.SemaphoreType.DMA((size // block,)),
            pltpu.SemaphoreType.DMA((cuts,)),
        ],
        cost_estimate=pl.CostEstimate(
            flops=6 * n * examples * row_count * size,
            bytes_accessed=4 * (n * examples + row_count) * size,
            transcendentals=0,
        ),
        compiler_params=pltpu.CompilerParams(vmem_limit_bytes=40 << 20),
        name="gram_rows",
    )(first, *[x for piece in parts for x in piece])


def body(hidden, out_grad, proj_in, proj_out, segment_ids):
    width = proj_in.shape[0]
    proj_size = width * width
    data = lax.axis_size("dp")
    model = lax.axis_size("mp")
    row_count = proj_size // (data * model)
    axes = ("dp", "mp")
    pair = 2 if data % 2 == 0 else 1
    groups = data // pair

    def owner(d):
        return min((model - 1) // 2 + d % pair, model - 1)

    def at(d, m):
        return d * model + (owner(d) + m) % model

    def hops(m):
        return max(abs((owner(d) + m) % model - owner(d)) for d in range(pair))

    others = sorted(range(1, model), key=hops)

    def to_owner(x):
        return [x] + [
            lax.ppermute(x, axes, [(at(d, m), at(d, 0)) for d in range(data)])
            for m in others
        ]

    def from_owner(x):
        return [
            lax.ppermute(x, axes, [(at(d, 0), at(d, m)) for d in range(data)])
            for m in others
        ]

    def other(g, k):
        return g ^ k if groups & (groups - 1) == 0 else (g + k) % groups

    def across(x, k):
        return lax.ppermute(
            x,
            "dp",
            [
                (g * pair + c, other(g, k) * pair + c)
                for g in range(groups)
                for c in range(pair)
            ],
        )

    def swap(x):
        return lax.ppermute(x, "dp", [(d, d ^ 1) for d in range(data)])

    d, m = lax.axis_index("dp"), lax.axis_index("mp")
    is_owner = m == jnp.minimum((model - 1) // 2 + d % pair, model - 1)

    tokens = hidden.shape[0]
    unit = tokens // 8
    (outputs,) = project(out_grad, proj_out, [4 * unit, 4 * unit], (tokens,))
    outputs_sent = to_owner(outputs)
    inputs = project(hidden, proj_in, [2 * unit] * 4, (6 * unit, 2 * unit))
    early = to_owner(inputs[0])
    late = to_owner(inputs[1])
    left, scale = expand(segment_ids, outputs_sent, EX_DEV)
    (sums,) = outer_sums(left, scale, early, 0, None, 0)
    pieces = []
    for summed in outer_sums(left, scale, late, 6 * unit, sums, 2):
        features = jnp.where(is_owner, summed, sum(from_owner(summed)))
        parts = [features] + [across(features, k) for k in sorted(range(1, groups), key=lambda k: -bin(k).count("1"))]
        if pair == 2:
            parts = parts + [swap(x) for x in parts]
        pieces.append(parts)
    first = ((d * model + m) * row_count).astype(jnp.int32).reshape(1)
    features, gram = gram_rows(first, list(zip(*pieces)), row_count)
    return features, gram


def solution(mesh):
    placed = (P("dp", "mp"), P("dp", "mp"), P(None, "mp"), P(None, "mp"), P("dp", None))
    return jax.shard_map(
        body,
        mesh=mesh,
        in_specs=placed,
        out_specs=(P("dp", None), P(("dp", "mp"), None)),
        check_vma=False,
    )
```

```python
import functools

import jax
import jax.numpy as jnp
from jax import lax
from jax.experimental import pallas as pl
from jax.experimental.pallas import tpu as pltpu
from jax.sharding import PartitionSpec as P


EX_DEV = 16
NT = (((1,), (1,)), ((), ()))
HBM = pl.BlockSpec(memory_space=pltpu.HBM)
VMEM = pl.BlockSpec(memory_space=pltpu.VMEM)
SMEM = pl.BlockSpec(memory_space=pltpu.SMEM)


def in_hbm(x):
    return pltpu.with_memory_space_constraint(x, pltpu.HBM)


def in_vmem(x):
    return pltpu.with_memory_space_constraint(x, pltpu.VMEM)


def project_kernel(blocks, cuts, x_ref, w_ref, *refs):
    out_refs = refs[: len(cuts)]
    x_buf, w_buf, x_sem, w_sem = refs[len(cuts) :]
    n = len(blocks)
    weights = pltpu.make_async_copy(w_ref, w_buf, w_sem)
    weights.start()
    copies = [
        pltpu.make_async_copy(
            x_ref.at[pl.ds(first, rows)], x_buf.at[pl.ds(first, rows)], x_sem.at[i]
        )
        for i, (first, rows) in enumerate(blocks)
    ]

    for copy in copies[:2]:
        copy.start()
    weights.wait()
    for i, (first, rows) in enumerate(blocks):
        copies[i].wait()
        if i + 2 < n:
            copies[i + 2].start()
        product = lax.dot_general(
            w_buf[...], x_buf[pl.ds(first, rows)], NT, preferred_element_type=jnp.float32
        )
        begin = 0
        for cut, out_ref in zip(cuts, out_refs):
            if begin <= first < begin + cut:
                out_ref[:, first - begin : first - begin + rows] = product
            begin += cut


def project(x, w, blocks, cuts):
    tokens, depth = x.shape
    width = w.shape[0]
    firsts = [sum(blocks[:i]) for i in range(len(blocks))]
    return pl.pallas_call(
        functools.partial(project_kernel, list(zip(firsts, blocks)), cuts),
        in_specs=[HBM, HBM],
        out_specs=[VMEM] * len(cuts),
        out_shape=[pltpu.VMEM((width, cut), jnp.float32) for cut in cuts],
        scratch_shapes=[
            pltpu.VMEM((tokens, depth), x.dtype),
            pltpu.VMEM((width, depth), w.dtype),
            pltpu.SemaphoreType.DMA((len(blocks),)),
            pltpu.SemaphoreType.DMA,
        ],
        cost_estimate=pl.CostEstimate(
            flops=2 * tokens * depth * width,
            bytes_accessed=2 * tokens * depth,
            transcendentals=0,
        ),
        compiler_params=pltpu.CompilerParams(vmem_limit_bytes=24 << 20),
        name="project",
    )(in_hbm(x), in_hbm(w))


def split(x):
    high = x.astype(jnp.bfloat16)
    return high, (x - high.astype(jnp.float32)).astype(jnp.bfloat16)


def total(refs):
    return sum((r[...] for r in refs[1:]), refs[0][...])


def expand_kernel(n, examples, seg_ref, *refs):
    out_ref, scale_ref = refs[n:]
    tokens = seg_ref.shape[1]
    outputs = total(refs[:n])
    mask = (
        seg_ref[...] == lax.broadcasted_iota(jnp.int32, (examples, tokens), 0)
    ).astype(jnp.float32)
    high = outputs.astype(jnp.bfloat16).astype(jnp.float32)
    low = outputs - high
    width = outputs.shape[0]
    half = width * examples
    for i in range(width):
        first = i * examples
        rows = slice(first, first + examples)
        out_ref[rows, :] = (high[i : i + 1, :] * mask).astype(jnp.bfloat16)
        rows = slice(half + first, half + first + examples)
        out_ref[rows, :] = (low[i : i + 1, :] * mask).astype(jnp.bfloat16)
    scale_ref[...] = jnp.broadcast_to(
        1.0 / jnp.sqrt(jnp.sum(mask, axis=1, keepdims=True)), scale_ref.shape
    )


def expand(segment_ids, parts, examples):
    width, tokens = parts[0].shape
    n = len(parts)
    return pl.pallas_call(
        functools.partial(expand_kernel, n, examples),
        in_specs=[VMEM] * (1 + n),
        out_specs=[VMEM] * 2,
        out_shape=[
            pltpu.VMEM((2 * width * examples, tokens), jnp.bfloat16),
            pltpu.VMEM((examples, 128), jnp.float32),
        ],
        cost_estimate=pl.CostEstimate(
            flops=4 * width * examples * tokens,
            bytes_accessed=4 * width * examples * tokens,
            transcendentals=0,
        ),
        compiler_params=pltpu.CompilerParams(vmem_limit_bytes=24 << 20),
        name="expand",
    )(segment_ids, *parts)


def outer_kernel(n, examples, first, last, left_ref, scale_ref, *refs):
    if first > 0:
        before_ref, *refs = refs
    input_refs, out_refs = refs[:n], refs[n:]
    width, tokens = input_refs[0].shape
    right = jnp.concatenate(split(total(input_refs)), axis=0)
    scale = scale_ref[:, :width]
    half = width * examples
    rank = width // len(out_refs)
    rows = rank * examples
    for k, out_ref in enumerate(out_refs):

        def dot(row):
            return lax.dot_general(
                left_ref[row : row + rows, first : first + tokens],
                right,
                NT,
                preferred_element_type=jnp.float32,
            )

        high, low = dot(k * rows), dot(half + k * rows)
        sums = high[:, :width] + high[:, width:] + low[:, :width] + low[:, width:]
        if first > 0:
            sums = sums + before_ref[k * rows : (k + 1) * rows, :]
        if not last:
            out_ref[...] = sums
            continue
        for i in range(rank):
            out_ref[:, i * width : (i + 1) * width] = (
                sums[i * examples : (i + 1) * examples] * scale
            )


def outer_sums(left, scale, inputs, first, before, cuts):
    examples = scale.shape[0]
    rows = left.shape[0]
    width, tokens = inputs[0].shape
    n = len(inputs)
    shapes = [(examples, width * width // cuts)] * cuts if cuts else [(width * examples, width)]
    operands = [left, scale] + ([before] if first > 0 else [])
    return pl.pallas_call(
        functools.partial(outer_kernel, n, examples, first, bool(cuts)),
        in_specs=[VMEM] * (len(operands) + n),
        out_specs=[VMEM] * len(shapes),
        out_shape=[pltpu.VMEM(shape, jnp.float32) for shape in shapes],
        cost_estimate=pl.CostEstimate(
            flops=4 * rows * tokens * width,
            bytes_accessed=2 * rows * tokens,
            transcendentals=0,
        ),
        compiler_params=pltpu.CompilerParams(vmem_limit_bytes=24 << 20),
        name="outer_sums",
    )(*[in_vmem(x) for x in operands], *inputs)


def gram_kernel(n, cuts, row_count, examples, scale, block, last, first_ref, *refs):
    parts = refs[: n * cuts]
    if last:
        before_ref, out_ref, terms, rows_ref, out_sem = refs[n * cuts :]
    else:
        features_ref, rows_ref, terms, features_sem = refs[n * cuts :]
    size = parts[0].shape[1]
    total_examples = n * examples
    copies = []
    if not last:
        copies = [
            pltpu.make_async_copy(
                parts[c], features_ref.at[:, pl.ds(c * size, size)], features_sem.at[c]
            )
            for c in range(cuts)
        ]
    for copy in copies:
        copy.start()
    for k in range(n):
        high = slice(k * examples, (k + 1) * examples)
        low = slice(total_examples + k * examples, total_examples + (k + 1) * examples)
        for c in range(cuts):
            columns = slice(c * size, (c + 1) * size)
            terms[high, columns], terms[low, columns] = split(parts[k * cuts + c][...])
    lanes = rows_ref.shape[0]
    first = first_ref[0]
    base = pl.multiple_of(first // lanes * lanes, lanes)
    left_high = terms[:total_examples, pl.ds(base, lanes)].T
    left_low = terms[total_examples:, pl.ds(base, lanes)].T
    left = jnp.concatenate([left_high, left_high, left_low], axis=1)
    offset = pl.multiple_of(first - base, row_count)

    for k in range(size * cuts // block):
        columns = slice(k * block, (k + 1) * block)
        right = jnp.concatenate([terms[:, columns], terms[:total_examples, columns]], axis=0)
        product = lax.dot_general(
            left, right, (((1,), (0,)), ((), ())), preferred_element_type=jnp.float32
        )
        if not last:
            rows_ref[:, columns] = product
            continue
        rows_ref[:, columns] = (before_ref[:, columns] + product) * scale
        copies.append(
            pltpu.make_async_copy(
                rows_ref.at[pl.ds(offset, row_count), columns], out_ref.at[:, columns], out_sem.at[k]
            )
        )
        copies[-1].start()
    for copy in copies:
        copy.wait()


def gram_rows(first, parts, row_count, examples, before):
    n, cuts = len(parts), len(parts[0])
    group = parts[0][0].shape[0]
    size = sum(x.shape[1] for x in parts[0])
    block = size // 4 if size % 512 == 0 else size
    rows = max(row_count, 128)
    last = before is not None
    scratch = [pltpu.VMEM((2 * n * group, size), jnp.bfloat16)]
    if last:
        out_specs = [HBM]
        out_shape = [jax.ShapeDtypeStruct((row_count, size), jnp.float32)]
        scratch += [
            pltpu.VMEM((rows, size), jnp.float32),
            pltpu.SemaphoreType.DMA((size // block,)),
        ]
    else:
        out_specs = [HBM, VMEM]
        out_shape = [
            jax.ShapeDtypeStruct((group, size), jnp.float32),
            pltpu.VMEM((rows, size), jnp.float32),
        ]
        scratch += [pltpu.SemaphoreType.DMA((cuts,))]
    operands = [x for piece in parts for x in piece] + ([in_vmem(before)] if last else [])
    return pl.pallas_call(
        functools.partial(
            gram_kernel, n, cuts, row_count, group, 1.0 / examples, block, last
        ),
        in_specs=[SMEM] + [VMEM] * len(operands),
        out_specs=out_specs,
        out_shape=out_shape,
        scratch_shapes=scratch,
        cost_estimate=pl.CostEstimate(
            flops=6 * n * group * row_count * size,
            bytes_accessed=4 * (n * group + row_count) * size,
            transcendentals=0,
        ),
        compiler_params=pltpu.CompilerParams(vmem_limit_bytes=40 << 20),
        name="gram_rows",
    )(first, *operands)


def body(hidden, out_grad, proj_in, proj_out, segment_ids):
    width = proj_in.shape[0]
    proj_size = width * width
    data = lax.axis_size("dp")
    model = lax.axis_size("mp")
    row_count = proj_size // (data * model)
    axes = ("dp", "mp")
    pair = 2 if data % 2 == 0 else 1
    groups = data // pair

    def owner(d):
        return min((model - 1) // 2 + d % pair, model - 1)

    def at(d, m):
        return d * model + (owner(d) + m) % model

    def hops(m):
        return max(abs((owner(d) + m) % model - owner(d)) for d in range(pair))

    others = sorted(range(1, model), key=hops)

    def to_owner(x):
        return [x] + [
            lax.ppermute(x, axes, [(at(d, m), at(d, 0)) for d in range(data)])
            for m in others
        ]

    def from_owner(x):
        return [
            lax.ppermute(x, axes, [(at(d, 0), at(d, m)) for d in range(data)])
            for m in sorted(others, key=hops, reverse=True)
        ]

    def other(g, k):
        return g ^ k if groups & (groups - 1) == 0 else (g + k) % groups

    def across(x, k):
        return lax.ppermute(
            x,
            "dp",
            [
                (g * pair + c, other(g, k) * pair + c)
                for g in range(groups)
                for c in range(pair)
            ],
        )

    def swap(x):
        return lax.ppermute(x, "dp", [(d, d ^ 1) for d in range(data)])

    d, m = lax.axis_index("dp"), lax.axis_index("mp")
    is_owner = m == jnp.minimum((model - 1) // 2 + d % pair, model - 1)

    tokens = hidden.shape[0]
    unit = tokens // 8
    (outputs,) = project(out_grad, proj_out, [4 * unit, 4 * unit], (tokens,))
    outputs_sent = to_owner(outputs)
    inputs = project(hidden, proj_in, [2 * unit] * 4, (6 * unit, 2 * unit))
    early = to_owner(inputs[0])
    late = to_owner(inputs[1])
    left, scale = expand(segment_ids, outputs_sent, EX_DEV)
    (sums,) = outer_sums(left, scale, early, 0, None, 0)
    pieces, swapped = [], []
    order = sorted(range(1, groups), key=lambda k: -bin(k).count("1"))
    for summed in outer_sums(left, scale, late, 6 * unit, sums, 2):
        features = jnp.where(is_owner, summed, sum(from_owner(summed)))
        parts = [features] + [across(features, k) for k in order]
        pieces.append(parts)
        swapped.append([swap(x) for x in parts] if pair == 2 else parts)
    first = ((d * model + m) * row_count).astype(jnp.int32).reshape(1)
    examples = EX_DEV * data
    features, gram = gram_rows(first, list(zip(*pieces)), row_count, examples, None)
    if pair == 2:
        (gram,) = gram_rows(first, list(zip(*swapped)), row_count, examples, gram)
    return features, gram


def solution(mesh):
    placed = (P("dp", "mp"), P("dp", "mp"), P(None, "mp"), P(None, "mp"), P("dp", None))
    return jax.shard_map(
        body,
        mesh=mesh,
        in_specs=placed,
        out_specs=(P("dp", None), P(("dp", "mp"), None)),
        check_vma=False,
    )
```
